32 devices in a mesh: trial: 2 (over core), bank: 4 (over y, x), zero: 4 (over z).
Axes of the slice: x: 2, y: 2, z: 4, core: 2. Of those that a mesh axis runs over, the one named last changes fastest.
Arguments:
- w_gate: float32 [128, 2048, 1024], P(('trial', 'bank'), 'zero'), parts along dimension 0, may hold values from -0.1875 to 0.1875
- w_up: float32 [128, 2048, 1024], P(('trial', 'bank'), 'zero'), parts along dimension 0, may hold values from -0.1875 to 0.1875
- router_weight: float32 [4096, 64], P(('trial', 'zero'), 'bank'), parts along dimension 0, may hold values from -0.125 to 0.125
- router_gain: float32 [4096], P(('trial', 'zero')), parts along dimension 0, may hold values from 0.25 to 1.75
Outputs:
- serve_gate: bfloat16 [128, 2048, 1024], P(('trial', 'bank'), None, 'zero'), parts along dimension 0
- serve_up: bfloat16 [128, 2048, 1024], P(('trial', 'bank'), None, 'zero'), parts along dimension 0
- scale_gate: float32 [128, 1024], P(('trial', 'bank'), 'zero'), parts along dimension 0
- scale_up: float32 [128, 1024], P(('trial', 'bank'), 'zero'), parts along dimension 0
- serve_router: bfloat16 [4096, 64], P('trial'), parts along dimension 0
The draws below stay inside these ranges and needn't reach their ends.
There are 2 independent parts, one for each index of `trial`. The reference program is written for one: setup_inputs(seed, part) draws one part's arguments, and reference() takes and returns one part's arrays. A program takes and returns all parts, laid end to end along the dimension named above; each array names one. Nothing has to cross between parts.
All inputs are finite; a program needn't handle non-finite values. Where the reference program divides by a largest or mean magnitude, that divisor is 1e-20 or more.
Results may differ from the reference program's by a relative error of at most 0.001.
Values may be sent and summed in bfloat16 or wider, within the bound.
A program may use at most 192 MiB of HBM per device.

```python
import jax
import jax.numpy as jnp

EXPERTS = 64
D_MODEL = 2048
D_EXPERT = 1024


def spiked(drawn, key, source, target, parts, factor):
    def block_of(position):
        return (jnp.arange(drawn.shape[position]) // (drawn.shape[position] // parts)).reshape((-1,) + (1,) * (drawn.ndim - 1 - position))

    near = jax.random.permutation(key, parts)[block_of(target)]
    other_side = (block_of(target) + parts // 2) % parts
    return jnp.where((block_of(source) == near) | (block_of(source) == other_side), factor * drawn, drawn)


def level_of(stream_key, dims, cuts, least, top_value):
    def one(dim, parts):
        heights = jax.random.uniform(jax.random.fold_in(jax.random.fold_in(stream_key, 6), dim), (parts,), jnp.float32, least / len(cuts), top_value / len(cuts))
        return jnp.repeat(jnp.exp(heights), dims[dim] // parts).reshape((-1,) + (1,) * (len(dims) - dim - 1))

    gain = one(*cuts[0])
    for cut in cuts[1:]:
        gain = gain * one(*cut)
    return gain


def noise(stream_key, dims, spread, bound, shards=(), held_as=jnp.bfloat16):
    gain = level_of(stream_key, dims, shards, -0.22, 0.18) if shards else 1.0
    entries = jax.random.normal(stream_key, dims, jnp.float32) * spread * gain
    return jnp.minimum(jnp.maximum(entries, -bound), bound).astype(held_as)


def noise_with(rng, extent, width, most, cuts, heavy, kind=jnp.bfloat16):
    array = width * jax.random.normal(rng, extent, jnp.float32)
    if cuts:
        array = array * level_of(rng, extent, cuts, -0.22, 0.18)
    return jnp.clip(spiked(array, jax.random.fold_in(rng, 3), *heavy), -most, most).astype(kind)


def setup_inputs(seed: int = 0, part: int = 0) -> dict:
    arg_keys = jax.random.split(jax.random.key(seed), 5)
    part_splits = jax.random.split(jax.random.fold_in(arg_keys[4], part), 5)
    return {
        "w_gate": noise_with(part_splits[0], (EXPERTS, D_MODEL, D_EXPERT), D_MODEL ** -0.5, 0.1875, ((0, 4), (1, 4)), (1, 2, 4, 2.0), jnp.float32),
        "w_up": noise_with(part_splits[1], (EXPERTS, D_MODEL, D_EXPERT), D_MODEL ** -0.5, 0.1875, ((0, 4), (1, 4)), (1, 2, 4, 2.0), jnp.float32),
        "router_weight": noise(part_splits[2], (D_MODEL, EXPERTS), D_MODEL ** -0.5, 0.125, ((0, 4), (1, 4)), jnp.float32),
        "router_gain": jnp.clip(1.0 + 0.15 * jax.random.normal(part_splits[3], (D_MODEL,), jnp.float32), 0.25, 1.75),
    }


def reference(w_gate, w_up, router_weight, router_gain):
    scale_gate = jnp.sum(jnp.abs(w_gate), axis=1) / D_MODEL
    serve_gate = (w_gate / jnp.expand_dims(scale_gate, 1)).astype(jnp.bfloat16)
    scale_up = jnp.sum(jnp.abs(w_up), axis=1) / D_MODEL
    serve_up = (w_up / jnp.expand_dims(scale_up, 1)).astype(jnp.bfloat16)
    serve_router = (router_weight * router_gain[:, None]).astype(jnp.bfloat16)
    return serve_gate, serve_up, scale_gate, scale_up, serve_router
```

```python
import functools

import jax
import jax.numpy as jnp
from jax import lax
from jax.experimental import pallas as pl
from jax.experimental.pallas import tpu as pltpu
from jax.sharding import PartitionSpec as P

MESH = pl.DeviceIdType.MESH
SLOTS = 3
STEP = 16
CUTS = 4
HEADS = 2


def plain(n, w_gate, w_up, router_weight, router_gain):
    d_model = w_gate.shape[1] * n

    def rescaled(w):
        scale = lax.psum(jnp.sum(jnp.abs(w), axis=1), "zero") / d_model
        narrow = (w / jnp.expand_dims(scale, 1)).astype(jnp.bfloat16)
        serve = lax.all_to_all(narrow, "zero", split_axis=2, concat_axis=1, tiled=True)
        width = serve.shape[2]
        return serve, lax.dynamic_slice_in_dim(scale, lax.axis_index("zero") * width, width, axis=1)

    serve_gate, scale_gate = rescaled(w_gate)
    serve_up, scale_up = rescaled(w_up)
    part = (router_weight * router_gain[:, None]).astype(jnp.bfloat16)
    row = lax.all_gather(part, "zero", axis=0, tiled=True)
    router = lax.all_gather(row, "bank", axis=1, tiled=True)
    return serve_gate, serve_up, scale_gate, scale_up, router


def kernel(
    n, banks, wg_ref, wu_ref, rw_ref, rg_ref, *refs
):
    og_ref, ou_ref, sg_ref, su_ref, rt_ref = refs[:5]
    tails = refs[5 : 5 + n]
    stage, first, sendbuf, parts, sums, lower, half, across, totals, scales = refs[5 + n : 15 + n]
    (
    tail_sem, in_sem, first_sem, own_sem, send_sem, recv_sem, x_send, x_recv, up_send, up_recv, mid_send, mid_recv,
    down_send, down_recv, rz_send, rz_recv, rb_send, rb_recv,
    ) = refs[15 + n :]
    me = lax.axis_index("zero")
    bank = lax.axis_index("bank")
    lead = lax.rem(lax.axis_index("trial"), 2) == 0
    w, o, so = (wg_ref, wu_ref), (og_ref, ou_ref), (sg_ref, su_ref)
    experts, rows, cols = wg_ref.shape
    width = cols // n
    d_model = rows * n
    last = experts - 1
    piece = rows // CUTS
    heads = [(m, e) for e in range(HEADS) for m in range(2)]

    def head(m, e, c):
        at = pl.ds(c * piece, piece)
        return pltpu.make_async_copy(w[m].at[e, at], first.at[m, e, at], first_sem.at[m, e, c])

    def load(m, e, slot):
        return pltpu.make_async_copy(w[m].at[e], stage.at[m, slot], in_sem.at[m, slot])

    def refill():
        for e in range(HEADS, min(HEADS + SLOTS, experts)):
            for m in range(2):
                load(m, e, e % SLOTS).start()

    for m, e in heads[:2]:
        for c in range(CUTS):
            head(m, e, c).start()

    def others(axis, here, count, act):
        for p in range(count):
            @pl.when(here != p)
            def _():
                act(p)

    barrier = pltpu.get_barrier_semaphore()

    def greet(axis):
        return lambda p: pl.semaphore_signal(barrier, inc=1, device_id={axis: p}, device_id_type=MESH)

    others("zero", me, n, greet("zero"))
    others("bank", bank, banks, greet("bank"))

    def sizes_of(src, count, acc):
        def body(r, acc):
            return acc + jnp.abs(src[pl.ds(pl.multiple_of(r * 8, 8), 8), :])

        return lax.fori_loop(0, count // 8, body, acc, unroll=8)

    empty = jnp.zeros((8, cols), jnp.float32)

    def head_sizes(m, e):
        acc = empty
        for c in range(CUTS):
            head(m, e, c).wait()
            acc = sizes_of(first.at[m, e, pl.ds(c * piece, piece)], piece, acc)
        parts[me, e, m] = jnp.sum(acc, axis=0, keepdims=True)

    def swap(m, e, s, p):
        return pltpu.make_async_remote_copy(
            src_ref=parts.at[s, e, m], dst_ref=parts.at[s, e, m],
            send_sem=x_send.at[m, e, p], recv_sem=x_recv.at[m, e, s],
            device_id={"zero": p}, device_id_type=MESH,
        )

    def arrived(m, e):
        others("zero", me, n, lambda p: swap(m, e, p, p).wait_recv())
        total = parts[0, e, m]
        for s in range(1, n):
            total = total + parts[s, e, m]
        totals[e, m] = total

    def narrow(src, m, e):
        scale = totals[e, m] / d_model
        factor = 1.0 / scale
        scales[...] = scale
        so[m][pl.ds(e, 1), :] = scales[:, pl.ds(pl.multiple_of(me * width, width), width)]

        def body(r, carry):
            at = pl.ds(pl.multiple_of(r * STEP, STEP), STEP)
            for c in range(n):
                lanes = slice(c * width, (c + 1) * width)
                sendbuf[m, e, c, at, :] = (src[at, lanes] * factor[:, lanes]).astype(jnp.bfloat16)
            return carry

        lax.fori_loop(0, rows // STEP, body, 0, unroll=2)

    def place(ref, e, s):
        return ref.at[e, pl.ds(pl.multiple_of(s * rows, rows), rows), :]

    def keep(m, e):
        pltpu.make_async_copy(sendbuf.at[m, e, me], place(o[m], e, me), own_sem.at[m]).start()

    def send(m, e, p):
        pltpu.make_async_remote_copy(
            src_ref=sendbuf.at[m, e, p], dst_ref=place(o[m], e, me),
            send_sem=send_sem.at[m, p], recv_sem=recv_sem.at[m, me],
            device_id={"zero": p}, device_id_type=MESH,
        ).start()

    def send_at(m, e, t):
        @pl.when(me + t < n)
        def _():
            send(m, e, me + t)

        @pl.when(me - t >= 0)
        def _():
            send(m, e, me - t)

    def send_all(m, e):
        for t in range(n - 1, 0, -1):
            send_at(m, e, t)

    for i, (m, e) in enumerate(heads):
        head_sizes(m, e)
        if i == 0:
            for later in heads[2:]:
                for c in range(CUTS):
                    head(*later, c).start()
            pl.semaphore_wait(barrier, n - 1 + banks - 1)
        others("zero", me, n, lambda p: swap(m, e, me, p).start())
        if i == 1:
            refill()

            @pl.when(lead)
            def _():
                for k in heads[:2]:
                    arrived(*k)
                    narrow(first.at[k], *k)
                    send_all(*k)
                    keep(*k)

    @pl.when(lead)
    def _():
        for k in heads[2:]:
            arrived(*k)
            narrow(first.at[k], *k)
            send_all(*k)
            keep(*k)

    depth = rw_ref.shape[1]
    mine = pl.ds(pl.multiple_of(me * depth, depth), depth)
    rt_ref[bank, :, mine] = (rw_ref[...] * rg_ref[...]).astype(jnp.bfloat16)

    def sizes(e, carry):
        slot = lax.rem(e, SLOTS)
        for m in range(2):
            load(m, e, slot).wait()
            acc = sizes_of(stage.at[m, slot], rows, empty)
            sums[e, m] = jnp.sum(acc, axis=0, keepdims=True)

            @pl.when(e + SLOTS < experts)
            def _():
                load(m, e + SLOTS, slot).start()
        return carry

    lax.fori_loop(HEADS, experts, sizes, 0)
    refill()

    span = pl.ds(HEADS, experts - HEADS)
    gates = (n // 2 - 1, n // 2)

    def members(g):
        side = range(n // 2) if g < n // 2 else range(n // 2, n)
        return [(i, p) for i, p in enumerate(p for p in side if p != g)]

    def rise(g, i):
        return pltpu.make_async_remote_copy(
            src_ref=sums.at[span], dst_ref=lower.at[i, span], send_sem=up_send, recv_sem=up_recv.at[i],
            device_id={"zero": g}, device_id_type=MESH,
        )

    def meet(g):
        return pltpu.make_async_remote_copy(
            src_ref=half.at[span], dst_ref=across.at[span], send_sem=mid_send, recv_sem=mid_recv,
            device_id={"zero": n - 1 - g}, device_id_type=MESH,
        )

    def give(i, p):
        return pltpu.make_async_remote_copy(
            src_ref=totals.at[span], dst_ref=totals.at[span], send_sem=down_send.at[i], recv_sem=down_recv,
            device_id={"zero": p}, device_id_type=MESH,
        )

    for g in gates:
        for i, p in members(g):
            @pl.when(me == p)
            def _():
                rise(g, i).start()

    @pl.when(jnp.logical_not(lead))
    def _():
        for k in heads:
            arrived(*k)
            narrow(first.at[k], *k)

    for g in gates:
        @pl.when(me == g)
        def _():
            total = sums[span]
            for i, p in members(g):
                rise(g, i).wait_recv()
                total = total + lower[i, span]
            half[span] = total
            meet(g).start()
            meet(g).wait_recv()
            totals[span] = half[span] + across[span]
            for i, p in members(g):
                give(i, p).start()

        for i, p in members(g):
            @pl.when(me == p)
            def _():
                give(i, p).wait_recv()

    def row_copy(s, p):
        at = pl.ds(pl.multiple_of(s * depth, depth), depth)
        return pltpu.make_async_remote_copy(
            src_ref=rt_ref.at[bank, :, at], dst_ref=rt_ref.at[bank, :, at],
            send_sem=rz_send.at[p], recv_sem=rz_recv.at[s],
            device_id={"zero": p}, device_id_type=MESH,
        )

    others("zero", me, n, lambda p: row_copy(me, p).start())

    @pl.when(jnp.logical_not(lead))
    def _():
        for k in heads:
            send_all(*k)
            keep(*k)

    def put(m, d):
        return pltpu.make_async_copy(
            sendbuf.at[m, last, lax.rem(me + d, n)], tails[d].at[m], tail_sem.at[d, m]
        )

    def narrowed(e, carry):
        slot = lax.rem(e, SLOTS)
        for m in range(2):
            load(m, e, slot).wait()
            narrow(stage.at[m, slot], m, e)

            @pl.when(e + SLOTS < experts)
            def _():
                load(m, e + SLOTS, slot).start()

            @pl.when(e < last)
            def _():
                send_at(m, e, 1)
                keep(m, e)
        return carry

    lax.fori_loop(HEADS, experts, narrowed, 0)
    for m in range(2):
        for d in range(n):
            put(m, d).start()

    def far(e, carry):
        for m in range(2):
            for t in range(2, n):
                send_at(m, e, t)
        return carry

    lax.fori_loop(HEADS, last, far, 0)
    for m in range(2):
        for d in range(n):
            put(m, d).wait()

    others("zero", me, n, lambda p: row_copy(p, p).wait_recv())

    def column_copy(s, p):
        return pltpu.make_async_remote_copy(
            src_ref=rt_ref.at[s], dst_ref=rt_ref.at[s],
            send_sem=rb_send.at[p], recv_sem=rb_recv.at[s],
            device_id={"bank": p}, device_id_type=MESH,
        )

    others("bank", bank, banks, lambda p: column_copy(bank, p).start())
    others("bank", bank, banks, lambda p: column_copy(p, p).wait_recv())
    others("bank", bank, banks, lambda p: column_copy(bank, p).wait_send())
    others("zero", me, n, lambda p: row_copy(me, p).wait_send())
    for m, e in heads:
        others("zero", me, n, lambda p: swap(m, e, me, p).wait_send())
    for g in gates:
        @pl.when(me == g)
        def _():
            meet(g).wait_send()
            for i, p in members(g):
                give(i, p).wait_send()

        for i, p in members(g):
            @pl.when(me == p)
            def _():
                rise(g, i).wait_send()

    for m in range(2):
        def whole(s, p):
            return pltpu.make_async_remote_copy(
                src_ref=sendbuf.at[m, pl.ds(0, last), p],
                dst_ref=o[m].at[:, pl.ds(pl.multiple_of(s * rows, rows), rows), :],
                send_sem=send_sem.at[m, p], recv_sem=recv_sem.at[m, s],
                device_id={"zero": p}, device_id_type=MESH,
            )

        pltpu.make_async_copy(
            sendbuf.at[m, pl.ds(0, last), me], o[m].at[:, pl.ds(pl.multiple_of(me * rows, rows), rows), :], own_sem.at[m]
        ).wait()
        others("zero", me, n, lambda p: whole(me, p).wait_send())
        others("zero", me, n, lambda p: whole(p, p).wait_recv())


def copy_kernel(n, a_ref, b_ref, own_ref, sa_ref, sb_ref, rt_ref, *outs):
    c_ref, d_ref = outs[:2]
    e = pl.program_id(0)
    rows = own_ref.shape[1]

    @pl.when(e < pl.num_programs(0) - 1)
    def _():
        c_ref[...] = a_ref[...]
        d_ref[...] = b_ref[...]

    @pl.when(e == 0)
    def _():
        for src, dst in zip((sa_ref, sb_ref, rt_ref), outs[2:]):
            dst[...] = src[...]

    @pl.when(e == pl.num_programs(0) - 1)
    def _():
        at = pl.ds(pl.multiple_of(lax.axis_index("zero") * rows, rows), rows)
        c_ref[0, at, :] = own_ref[0]
        d_ref[0, at, :] = own_ref[1]


def spread(n, og, ou, own, *small):
    main, height, width = og.shape
    block = pl.BlockSpec((1, height, width), lambda e: (e, 0, 0))
    front = pl.BlockSpec((1, height, width), lambda e: (jnp.minimum(e, main - 1), 0, 0))
    out = jax.ShapeDtypeStruct((main + 1, height, width), og.dtype)

    def all_of(a):
        return pl.BlockSpec(a.shape, lambda e: (0,) * a.ndim)

    return pl.pallas_call(
        functools.partial(copy_kernel, n),
        grid=(main + 1,),
        in_specs=[front, front] + [all_of(a) for a in (own, *small)],
        out_specs=(block, block, *[all_of(a) for a in small]),
        out_shape=(out, out, *[jax.ShapeDtypeStruct(a.shape, a.dtype) for a in small]),
        cost_estimate=pl.CostEstimate(flops=0, bytes_accessed=8 * og.size, transcendentals=0),
        name="spread",
    )(og, ou, own, *small)


def join_kernel(n, shifts, *refs):
    count = len(shifts)
    blocks, outs, sem = refs[2 : 2 + count], refs[2 + count : 4 + count], refs[4 + count]
    me = lax.axis_index("zero")
    last = outs[0].shape[0] - 1
    rows = blocks[0].shape[1]
    copies = []
    for i, d in enumerate(shifts):
        at = pl.ds(pl.multiple_of(lax.rem(me - d + n, n) * rows, rows), rows)
        for m in range(2):
            copies.append(pltpu.make_async_copy(blocks[i].at[m], outs[m].at[last, at, :], sem.at[i, m]))
    for copy in copies:
        copy.start()
    for copy in copies:
        copy.wait()


def join(n, shifts, og, ou, blocks):
    anywhere = pl.BlockSpec(memory_space=pl.ANY)
    vmem = pl.BlockSpec(memory_space=pltpu.VMEM)
    return pl.pallas_call(
        functools.partial(join_kernel, n, shifts),
        out_shape=(jax.ShapeDtypeStruct(og.shape, og.dtype), jax.ShapeDtypeStruct(ou.shape, ou.dtype)),
        in_specs=[anywhere, anywhere] + [vmem] * len(blocks),
        out_specs=(anywhere, anywhere),
        scratch_shapes=[pltpu.SemaphoreType.DMA((len(blocks), 2))],
        input_output_aliases={0: 0, 1: 1},
        compiler_params=pltpu.CompilerParams(vmem_limit_bytes=8 * 1024 * 1024),
        name="join",
    )(og, ou, *blocks)


def local(n, banks, w_gate, w_up, router_weight, router_gain):
    experts, rows, cols = w_gate.shape
    width = cols // n
    depth, heads = router_weight.shape
    fits = width % 128 == 0 and rows % (8 * CUTS) == 0 and depth % 128 == 0 and heads % 16 == 0
    fits = fits and experts > HEADS + 1 and n % 2 == 0
    if not fits:
        return plain(n, w_gate, w_up, router_weight, router_gain)
    anywhere = pl.BlockSpec(memory_space=pl.ANY)
    vmem = pl.BlockSpec(memory_space=pltpu.VMEM)
    dma = pltpu.SemaphoreType.DMA
    serve = jax.ShapeDtypeStruct((experts - 1, rows * n, width), jnp.bfloat16)
    tail = jax.ShapeDtypeStruct((2, rows, width), jnp.bfloat16)
    scale = jax.ShapeDtypeStruct((experts, width), jnp.float32)
    sizes = pltpu.VMEM((experts, 2, 1, cols), jnp.float32)
    og, ou, sg, su, rt, *tails = pl.pallas_call(
        functools.partial(kernel, n, banks),
        out_shape=(serve, serve, scale, scale, jax.ShapeDtypeStruct((banks, heads, depth * n), jnp.bfloat16), *[tail] * n),
        in_specs=[anywhere, anywhere, vmem, vmem],
        out_specs=(anywhere, anywhere, vmem, vmem, vmem, *[anywhere] * n),
        scratch_shapes=[
            pltpu.VMEM((2, SLOTS, rows, cols), jnp.float32),
            pltpu.VMEM((2, HEADS, rows, cols), jnp.float32),
            pltpu.VMEM((2, experts, n, rows, width), jnp.bfloat16),
            pltpu.VMEM((n, HEADS, 2, 1, cols), jnp.float32),
            sizes,
            pltpu.VMEM((max(n // 2 - 1, 1), experts, 2, 1, cols), jnp.float32),
            sizes, sizes, sizes,
            pltpu.VMEM((1, cols), jnp.float32),
            dma((n, 2)), dma((2, SLOTS)), dma((2, HEADS, CUTS)), dma((2,)), dma((2, n)), dma((2, n)),
            dma((2, HEADS, n)), dma((2, HEADS, n)), dma, dma((n,)), dma, dma, dma((n,)), dma,
            dma((n,)), dma((n,)), dma((banks,)), dma((banks,)),
        ],
        compiler_params=pltpu.CompilerParams(
            collective_id=0, has_side_effects=True, vmem_limit_bytes=58 * 1024 * 1024
        ),
    )(w_gate, w_up, router_weight.T, router_gain[None, :])
    arrived = [
        lax.ppermute(tails[d], "zero", [(i, (i + d) % n) for i in range(n)]) for d in range(1, n)
    ]
    og, ou, sg, su, rt = spread(n, og, ou, tails[0], sg, su, rt)
    if n > 2:
        og, ou = join(n, tuple(range(1, n - 1)), og, ou, arrived[:-1])
    og, ou = join(n, (n - 1,), og, ou, arrived[-1:])
    return og, ou, sg, su, rt.reshape(banks * heads, depth * n).T


def solution(mesh):
    n, banks = mesh.shape["zero"], mesh.shape["bank"]
    return jax.shard_map(
        functools.partial(local, n, banks),
        mesh=mesh,
        in_specs=(
            P(("trial", "bank"), "zero", None),
            P(("trial", "bank"), "zero", None),
            P(("trial", "zero"), "bank"),
            P(("trial", "zero")),
        ),
        out_specs=(
            P(("trial", "bank"), None, "zero"),
            P(("trial", "bank"), None, "zero"),
            P(("trial", "bank"), "zero"),
            P(("trial", "bank"), "zero"),
            P("trial", None),
        ),
        check_vma=False,
    )
```

```python
import functools

import jax
import jax.numpy as jnp
from jax import lax
from jax.experimental import pallas as pl
from jax.experimental.pallas import tpu as pltpu
from jax.sharding import PartitionSpec as P

MESH = pl.DeviceIdType.MESH
SLOTS = 3
STEP = 16
CUTS = 4
HEADS = 2
TAIL = 2


def plain(n, w_gate, w_up, router_weight, router_gain):
    d_model = w_gate.shape[1] * n

    def rescaled(w):
        scale = lax.psum(jnp.sum(jnp.abs(w), axis=1), "zero") / d_model
        narrow = (w / jnp.expand_dims(scale, 1)).astype(jnp.bfloat16)
        serve = lax.all_to_all(narrow, "zero", split_axis=2, concat_axis=1, tiled=True)
        width = serve.shape[2]
        return serve, lax.dynamic_slice_in_dim(scale, lax.axis_index("zero") * width, width, axis=1)

    serve_gate, scale_gate = rescaled(w_gate)
    serve_up, scale_up = rescaled(w_up)
    part = (router_weight * router_gain[:, None]).astype(jnp.bfloat16)
    row = lax.all_gather(part, "zero", axis=0, tiled=True)
    router = lax.all_gather(row, "bank", axis=1, tiled=True)
    return serve_gate, serve_up, scale_gate, scale_up, router


def kernel(
    n, banks, wg_ref, wu_ref, rw_ref, rg_ref, *refs
):
    og_ref, ou_ref, sg_ref, su_ref, rt_ref = refs[:5]
    tails = refs[5 : 5 + n]
    stage, first, sendbuf, parts, sums, lower, half, across, totals, scales, router, gain = refs[5 + n : 17 + n]
    (
    tail_sem, in_sem, first_sem, own_sem, send_sem, recv_sem, x_send, x_recv, up_send, up_recv, mid_send, mid_recv,
    down_send, down_recv, rz_send, rz_recv, rb_send, rb_recv, r_sem,
    ) = refs[17 + n :]
    me = lax.axis_index("zero")
    bank = lax.axis_index("bank")
    lead = lax.rem(lax.axis_index("trial"), 2) == 1
    w, o, so = (wg_ref, wu_ref), (og_ref, ou_ref), (sg_ref, su_ref)
    experts, rows, cols = wg_ref.shape
    width = cols // n
    d_model = rows * n
    main = experts - TAIL
    piece = rows // CUTS
    heads = [(m, e) for e in range(HEADS) for m in range(2)]

    def head(m, e, c):
        at = pl.ds(c * piece, piece)
        return pltpu.make_async_copy(w[m].at[e, at], first.at[m, e, at], first_sem.at[m, e, c])

    def load(m, e, slot):
        return pltpu.make_async_copy(w[m].at[e], stage.at[m, slot], in_sem.at[m, slot])

    def refill():
        for e in range(HEADS, min(HEADS + SLOTS, experts)):
            for m in range(2):
                load(m, e, e % SLOTS).start()

    for m, e in heads[:2]:
        for c in range(CUTS):
            head(m, e, c).start()
    small = [pltpu.make_async_copy(src, dst, r_sem.at[i]) for i, (src, dst) in enumerate(((rw_ref, router), (rg_ref, gain)))]
    for copy in small:
        copy.start()

    def others(axis, here, count, act):
        for p in range(count):
            @pl.when(here != p)
            def _():
                act(p)

    barrier = pltpu.get_barrier_semaphore()

    def greet(axis):
        return lambda p: pl.semaphore_signal(barrier, inc=1, device_id={axis: p}, device_id_type=MESH)

    others("zero", me, n, greet("zero"))
    others("bank", bank, banks, greet("bank"))

    def sizes_of(src, count, acc):
        def body(r, acc):
            return acc + jnp.abs(src[pl.ds(pl.multiple_of(r * 8, 8), 8), :])

        return lax.fori_loop(0, count // 8, body, acc, unroll=8)

    empty = jnp.zeros((8, cols), jnp.float32)

    def head_sizes(m, e):
        acc = empty
        for c in range(CUTS):
            head(m, e, c).wait()
            acc = sizes_of(first.at[m, e, pl.ds(c * piece, piece)], piece, acc)
        parts[me, e, m] = jnp.sum(acc, axis=0, keepdims=True)

    def swap(m, e, s, p):
        return pltpu.make_async_remote_copy(
            src_ref=parts.at[s, e, m], dst_ref=parts.at[s, e, m],
            send_sem=x_send.at[m, e, p], recv_sem=x_recv.at[m, e, s],
            device_id={"zero": p}, device_id_type=MESH,
        )

    def arrived(m, e):
        others("zero", me, n, lambda p: swap(m, e, p, p).wait_recv())
        total = parts[0, e, m]
        for s in range(1, n):
            total = total + parts[s, e, m]
        totals[e, m] = total

    def narrow(src, m, e):
        scale = totals[e, m] / d_model
        factor = 1.0 / scale
        scales[...] = scale
        so[m][pl.ds(e, 1), :] = scales[:, pl.ds(pl.multiple_of(me * width, width), width)]

        def body(r, carry):
            at = pl.ds(pl.multiple_of(r * STEP, STEP), STEP)
            for c in range(n):
                lanes = slice(c * width, (c + 1) * width)
                sendbuf[m, e, c, at, :] = (src[at, lanes] * factor[:, lanes]).astype(jnp.bfloat16)
            return carry

        lax.fori_loop(0, rows // STEP, body, 0, unroll=2)

    def place(ref, e, s):
        return ref.at[e, pl.ds(pl.multiple_of(s * rows, rows), rows), :]

    def keep(m, e):
        pltpu.make_async_copy(sendbuf.at[m, e, me], place(o[m], e, me), own_sem.at[m]).start()

    def send(m, e, p):
        pltpu.make_async_remote_copy(
            src_ref=sendbuf.at[m, e, p], dst_ref=place(o[m], e, me),
            send_sem=send_sem.at[m, p], recv_sem=recv_sem.at[m, me],
            device_id={"zero": p}, device_id_type=MESH,
        ).start()

    def send_at(m, e, t):
        @pl.when(me + t < n)
        def _():
            send(m, e, me + t)

        @pl.when(me - t >= 0)
        def _():
            send(m, e, me - t)

    def send_all(m, e):
        for t in range(n - 1, 0, -1):
            send_at(m, e, t)

    depth = rw_ref.shape[1]
    mine = pl.ds(pl.multiple_of(me * depth, depth), depth)
    for copy in small:
        copy.wait()
    rt_ref[bank, :, mine] = (router[...] * gain[...]).astype(jnp.bfloat16)

    def row_copy(s, p):
        at = pl.ds(pl.multiple_of(s * depth, depth), depth)
        return pltpu.make_async_remote_copy(
            src_ref=rt_ref.at[bank, :, at], dst_ref=rt_ref.at[bank, :, at],
            send_sem=rz_send.at[p], recv_sem=rz_recv.at[s],
            device_id={"zero": p}, device_id_type=MESH,
        )

    for i, (m, e) in enumerate(heads):
        head_sizes(m, e)
        if i == 0:
            for later in heads[2:]:
                for c in range(CUTS):
                    head(*later, c).start()
            pl.semaphore_wait(barrier, n - 1 + banks - 1)
        others("zero", me, n, lambda p: swap(m, e, me, p).start())
        if i == 1:
            others("zero", me, n, lambda p: row_copy(me, p).start())
            refill()

            @pl.when(lead)
            def _():
                for k in heads[:2]:
                    arrived(*k)
                    narrow(first.at[k], *k)
                    send_all(*k)
                    keep(*k)

    @pl.when(lead)
    def _():
        for k in heads[2:]:
            arrived(*k)
            narrow(first.at[k], *k)
            send_all(*k)
            keep(*k)

    def sizes(e, carry):
        slot = lax.rem(e, SLOTS)
        for m in range(2):
            load(m, e, slot).wait()
            acc = sizes_of(stage.at[m, slot], rows, empty)
            sums[e, m] = jnp.sum(acc, axis=0, keepdims=True)

            @pl.when(e + SLOTS < experts)
            def _():
                load(m, e + SLOTS, slot).start()
        return carry

    lax.fori_loop(HEADS, experts, sizes, 0)
    refill()

    span = pl.ds(HEADS, experts - HEADS)
    gates = (n // 2 - 1, n // 2)

    def members(g):
        side = range(n // 2) if g < n // 2 else range(n // 2, n)
        return [(i, p) for i, p in enumerate(p for p in side if p != g)]

    def rise(g, i):
        return pltpu.make_async_remote_copy(
            src_ref=sums.at[span], dst_ref=lower.at[i, span], send_sem=up_send, recv_sem=up_recv.at[i],
            device_id={"zero": g}, device_id_type=MESH,
        )

    def meet(g):
        return pltpu.make_async_remote_copy(
            src_ref=half.at[span], dst_ref=across.at[span], send_sem=mid_send, recv_sem=mid_recv,
            device_id={"zero": n - 1 - g}, device_id_type=MESH,
        )

    def give(i, p):
        return pltpu.make_async_remote_copy(
            src_ref=totals.at[span], dst_ref=totals.at[span], send_sem=down_send.at[i], recv_sem=down_recv,
            device_id={"zero": p}, device_id_type=MESH,
        )

    for g in gates:
        for i, p in members(g):
            @pl.when(me == p)
            def _():
                rise(g, i).start()

    @pl.when(jnp.logical_not(lead))
    def _():
        for k in heads:
            arrived(*k)
            narrow(first.at[k], *k)

    for g in gates:
        @pl.when(me == g)
        def _():
            total = sums[span]
            for i, p in members(g):
                rise(g, i).wait_recv()
                total = total + lower[i, span]
            half[span] = total
            meet(g).start()
            meet(g).wait_recv()
            totals[span] = half[span] + across[span]
            for i, p in members(g):
                give(i, p).start()

        for i, p in members(g):
            @pl.when(me == p)
            def _():
                give(i, p).wait_recv()

    def put(m, d):
        return pltpu.make_async_copy(
            sendbuf.at[m, pl.ds(main, TAIL), lax.rem(me + d, n)], tails[d].at[m], tail_sem.at[d, m]
        )

    def narrowed(e, carry):
        slot = lax.rem(e, SLOTS)
        for m in range(2):
            load(m, e, slot).wait()
            narrow(stage.at[m, slot], m, e)

            @pl.when(e + SLOTS < experts)
            def _():
                load(m, e + SLOTS, slot).start()

            @pl.when(e < main)
            def _():
                keep(m, e)

                @pl.when(lead)
                def _():
                    send_at(m, e, 1)
        return carry

    lax.fori_loop(HEADS, experts, narrowed, 0)
    for m in range(2):
        for d in range(n):
            put(m, d).start()

    @pl.when(jnp.logical_not(lead))
    def _():
        for k in heads:
            send_all(*k)
            keep(*k)

        def near(e, carry):
            for m in range(2):
                send_at(m, e, 1)
            return carry

        lax.fori_loop(HEADS, main, near, 0)

    def far(e, carry):
        for m in range(2):
            for t in range(2, n):
                send_at(m, e, t)
        return carry

    lax.fori_loop(HEADS, main, far, 0)
    for m in range(2):
        for d in range(n):
            put(m, d).wait()

    others("zero", me, n, lambda p: row_copy(p, p).wait_recv())

    def column_copy(s, p):
        return pltpu.make_async_remote_copy(
            src_ref=rt_ref.at[s], dst_ref=rt_ref.at[s],
            send_sem=rb_send.at[p], recv_sem=rb_recv.at[s],
            device_id={"bank": p}, device_id_type=MESH,
        )

    others("bank", bank, banks, lambda p: column_copy(bank, p).start())
    others("bank", bank, banks, lambda p: column_copy(p, p).wait_recv())
    others("bank", bank, banks, lambda p: column_copy(bank, p).wait_send())
    others("zero", me, n, lambda p: row_copy(me, p).wait_send())
    for m, e in heads:
        others("zero", me, n, lambda p: swap(m, e, me, p).wait_send())
    for g in gates:
        @pl.when(me == g)
        def _():
            meet(g).wait_send()
            for i, p in members(g):
                give(i, p).wait_send()

        for i, p in members(g):
            @pl.when(me == p)
            def _():
                rise(g, i).wait_send()

    for m in range(2):
        def whole(s, p):
            return pltpu.make_async_remote_copy(
                src_ref=sendbuf.at[m, pl.ds(0, main), p],
                dst_ref=o[m].at[:, pl.ds(pl.multiple_of(s * rows, rows), rows), :],
                send_sem=send_sem.at[m, p], recv_sem=recv_sem.at[m, s],
                device_id={"zero": p}, device_id_type=MESH,
            )

        pltpu.make_async_copy(
            sendbuf.at[m, pl.ds(0, main), me], o[m].at[:, pl.ds(pl.multiple_of(me * rows, rows), rows), :], own_sem.at[m]
        ).wait()
        others("zero", me, n, lambda p: whole(me, p).wait_send())
        others("zero", me, n, lambda p: whole(p, p).wait_recv())


def copy_kernel(n, a_ref, b_ref, own_ref, sa_ref, sb_ref, rt_ref, *outs):
    c_ref, d_ref = outs[:2]
    e = pl.program_id(0)
    tail, rows = own_ref.shape[1:3]
    main = pl.num_programs(0) - tail

    @pl.when(e < main)
    def _():
        c_ref[...] = a_ref[...]
        d_ref[...] = b_ref[...]

    @pl.when(e == 0)
    def _():
        for src, dst in zip((sa_ref, sb_ref, rt_ref), outs[2:]):
            dst[...] = src[...]

    @pl.when(e >= main)
    def _():
        at = pl.ds(pl.multiple_of(lax.axis_index("zero") * rows, rows), rows)
        c_ref[0, at, :] = own_ref[0, e - main]
        d_ref[0, at, :] = own_ref[1, e - main]


def spread(n, og, ou, own, *small):
    main, height, width = og.shape
    block = pl.BlockSpec((1, height, width), lambda e: (e, 0, 0))
    front = pl.BlockSpec((1, height, width), lambda e: (jnp.minimum(e, main - 1), 0, 0))
    experts = main + own.shape[1]
    out = jax.ShapeDtypeStruct((experts, height, width), og.dtype)

    def all_of(a):
        return pl.BlockSpec(a.shape, lambda e: (0,) * a.ndim)

    return pl.pallas_call(
        functools.partial(copy_kernel, n),
        grid=(experts,),
        in_specs=[front, front] + [all_of(a) for a in (own, *small)],
        out_specs=(block, block, *[all_of(a) for a in small]),
        out_shape=(out, out, *[jax.ShapeDtypeStruct(a.shape, a.dtype) for a in small]),
        cost_estimate=pl.CostEstimate(flops=0, bytes_accessed=8 * og.size, transcendentals=0),
        name="spread",
    )(og, ou, own, *small)


def join_kernel(n, shifts, *refs):
    count = len(shifts)
    blocks, outs, sem = refs[2 : 2 + count], refs[2 + count : 4 + count], refs[4 + count]
    me = lax.axis_index("zero")
    tail, rows = blocks[0].shape[1:3]
    ends = pl.ds(outs[0].shape[0] - tail, tail)
    copies = []
    for i, d in enumerate(shifts):
        at = pl.ds(pl.multiple_of(lax.rem(me - d + n, n) * rows, rows), rows)
        for m in range(2):
            copies.append(pltpu.make_async_copy(blocks[i].at[m], outs[m].at[ends, at, :], sem.at[i, m]))
    for copy in copies:
        copy.start()
    for copy in copies:
        copy.wait()


def join(n, shifts, og, ou, blocks):
    anywhere = pl.BlockSpec(memory_space=pl.ANY)
    vmem = pl.BlockSpec(memory_space=pltpu.VMEM)
    return pl.pallas_call(
        functools.partial(join_kernel, n, shifts),
        out_shape=(jax.ShapeDtypeStruct(og.shape, og.dtype), jax.ShapeDtypeStruct(ou.shape, ou.dtype)),
        in_specs=[anywhere, anywhere] + [vmem] * len(blocks),
        out_specs=(anywhere, anywhere),
        scratch_shapes=[pltpu.SemaphoreType.DMA((len(blocks), 2))],
        input_output_aliases={0: 0, 1: 1},
        compiler_params=pltpu.CompilerParams(vmem_limit_bytes=8 * 1024 * 1024),
        name="join",
    )(og, ou, *blocks)


def local(n, banks, w_gate, w_up, router_weight, router_gain):
    experts, rows, cols = w_gate.shape
    width = cols // n
    depth, heads = router_weight.shape
    fits = width % 128 == 0 and rows % (8 * CUTS) == 0 and depth % 128 == 0 and heads % 16 == 0
    fits = fits and experts > HEADS + TAIL and n % 2 == 0
    if not fits:
        return plain(n, w_gate, w_up, router_weight, router_gain)
    anywhere = pl.BlockSpec(memory_space=pl.ANY)
    vmem = pl.BlockSpec(memory_space=pltpu.VMEM)
    dma = pltpu.SemaphoreType.DMA
    serve = jax.ShapeDtypeStruct((experts - TAIL, rows * n, width), jnp.bfloat16)
    tail = jax.ShapeDtypeStruct((2, TAIL, rows, width), jnp.bfloat16)
    scale = jax.ShapeDtypeStruct((experts, width), jnp.float32)
    sizes = pltpu.VMEM((experts, 2, 1, cols), jnp.float32)
    og, ou, sg, su, rt, *tails = pl.pallas_call(
        functools.partial(kernel, n, banks),
        out_shape=(serve, serve, scale, scale, jax.ShapeDtypeStruct((banks, heads, depth * n), jnp.bfloat16), *[tail] * n),
        in_specs=[anywhere] * 4,
        out_specs=(anywhere, anywhere, vmem, vmem, vmem, *[anywhere] * n),
        scratch_shapes=[
            pltpu.VMEM((2, SLOTS, rows, cols), jnp.float32),
            pltpu.VMEM((2, HEADS, rows, cols), jnp.float32),
            pltpu.VMEM((2, experts, n, rows, width), jnp.bfloat16),
            pltpu.VMEM((n, HEADS, 2, 1, cols), jnp.float32),
            sizes,
            pltpu.VMEM((max(n // 2 - 1, 1), experts, 2, 1, cols), jnp.float32),
            sizes, sizes, sizes,
            pltpu.VMEM((1, cols), jnp.float32),
            pltpu.VMEM((heads, depth), jnp.float32),
            pltpu.VMEM((1, depth), jnp.float32),
            dma((n, 2)), dma((2, SLOTS)), dma((2, HEADS, CUTS)), dma((2,)), dma((2, n)), dma((2, n)),
            dma((2, HEADS, n)), dma((2, HEADS, n)), dma, dma((n,)), dma, dma, dma((n,)), dma,
            dma((n,)), dma((n,)), dma((banks,)), dma((banks,)), dma((2,)),
        ],
        compiler_params=pltpu.CompilerParams(
            collective_id=0, has_side_effects=True, vmem_limit_bytes=58 * 1024 * 1024
        ),
    )(w_gate, w_up, router_weight.T, router_gain[None, :])
    arrived = [
        lax.ppermute(tails[d], "zero", [(i, (i + d) % n) for i in range(n)]) for d in range(1, n)
    ]
    og, ou, sg, su, rt = spread(n, og, ou, tails[0], sg, su, rt)
    if n > 2:
        og, ou = join(n, tuple(range(1, n - 1)), og, ou, arrived[:-1])
    og, ou = join(n, (n - 1,), og, ou, arrived[-1:])
    return og, ou, sg, su, rt.reshape(banks * heads, depth * n).T


def solution(mesh):
    n, banks = mesh.shape["zero"], mesh.shape["bank"]
    return jax.shard_map(
        functools.partial(local, n, banks),
        mesh=mesh,
        in_specs=(
            P(("trial", "bank"), "zero", None),
            P(("trial", "bank"), "zero", None),
            P(("trial", "zero"), "bank"),
            P(("trial", "zero")),
        ),
        out_specs=(
            P(("trial", "bank"), None, "zero"),
            P(("trial", "bank"), None, "zero"),
            P(("trial", "bank"), "zero"),
            P(("trial", "bank"), "zero"),
            P("trial", None),
        ),
        check_vma=False,
    )
```

```python
import functools

import jax
import jax.numpy as jnp
from jax import lax
from jax.experimental import pallas as pl
from jax.experimental.pallas import tpu as pltpu
from jax.sharding import PartitionSpec as P

MESH = pl.DeviceIdType.MESH
SLOTS = 3
STEP = 16
CUTS = 4
HEADS = 2
TAIL = 2


def plain(n, w_gate, w_up, router_weight, router_gain):
    d_model = w_gate.shape[1] * n

    def rescaled(w):
        scale = lax.psum(jnp.sum(jnp.abs(w), axis=1), "zero") / d_model
        narrow = (w / jnp.expand_dims(scale, 1)).astype(jnp.bfloat16)
        serve = lax.all_to_all(narrow, "zero", split_axis=2, concat_axis=1, tiled=True)
        width = serve.shape[2]
        return serve, lax.dynamic_slice_in_dim(scale, lax.axis_index("zero") * width, width, axis=1)

    serve_gate, scale_gate = rescaled(w_gate)
    serve_up, scale_up = rescaled(w_up)
    part = (router_weight * router_gain[:, None]).astype(jnp.bfloat16)
    row = lax.all_gather(part, "zero", axis=0, tiled=True)
    router = lax.all_gather(row, "bank", axis=1, tiled=True)
    return serve_gate, serve_up, scale_gate, scale_up, router


def kernel(
    n, banks, wg_ref, wu_ref, rw_ref, rg_ref, *refs
):
    og_ref, ou_ref, sg_ref, su_ref, rt_ref = refs[:5]
    tails = refs[5 : 5 + n]
    stage, first, sendbuf, parts, sums, lower, half, across, totals, scales, router, gain = refs[5 + n : 17 + n]
    (
    tail_sem, in_sem, first_sem, own_sem, send_sem, recv_sem, x_send, x_recv, up_send, up_recv, mid_send, mid_recv,
    down_send, down_recv, rz_send, rz_recv, rb_send, rb_recv, r_sem,
    ) = refs[17 + n :]
    me = lax.axis_index("zero")
    bank = lax.axis_index("bank")
    lead = lax.rem(lax.axis_index("trial"), 2) == 1
    w, o, so = (wg_ref, wu_ref), (og_ref, ou_ref), (sg_ref, su_ref)
    experts, rows, cols = wg_ref.shape
    width = cols // n
    d_model = rows * n
    main = experts - TAIL
    piece = rows // CUTS
    heads = [(m, e) for e in range(HEADS) for m in range(2)]

    def head(m, e, c):
        at = pl.ds(c * piece, piece)
        return pltpu.make_async_copy(w[m].at[e, at], first.at[m, e, at], first_sem.at[m, e, c])

    def load(m, e, slot):
        return pltpu.make_async_copy(w[m].at[e], stage.at[m, slot], in_sem.at[m, slot])

    def refill():
        for e in range(HEADS, min(HEADS + SLOTS, experts)):
            for m in range(2):
                load(m, e, e % SLOTS).start()

    for m, e in heads[:2]:
        for c in range(CUTS):
            head(m, e, c).start()
    small = [pltpu.make_async_copy(src, dst, r_sem.at[i]) for i, (src, dst) in enumerate(((rw_ref, router), (rg_ref, gain)))]
    for copy in small:
        copy.start()

    def others(axis, here, count, act):
        for p in range(count):
            @pl.when(here != p)
            def _():
                act(p)

    barrier = pltpu.get_barrier_semaphore()

    def greet(axis):
        return lambda p: pl.semaphore_signal(barrier, inc=1, device_id={axis: p}, device_id_type=MESH)

    others("zero", me, n, greet("zero"))
    others("bank", bank, banks, greet("bank"))

    def sizes_of(src, count, acc):
        def body(r, acc):
            return acc + jnp.abs(src[pl.ds(pl.multiple_of(r * 8, 8), 8), :])

        return lax.fori_loop(0, count // 8, body, acc, unroll=8)

    empty = jnp.zeros((8, cols), jnp.float32)

    def head_sizes(m, e):
        acc = empty
        for c in range(CUTS):
            head(m, e, c).wait()
            acc = sizes_of(first.at[m, e, pl.ds(c * piece, piece)], piece, acc)
        parts[me, e, m] = jnp.sum(acc, axis=0, keepdims=True)

    def swap(m, e, s, p):
        return pltpu.make_async_remote_copy(
            src_ref=parts.at[s, e, m], dst_ref=parts.at[s, e, m],
            send_sem=x_send.at[m, e, p], recv_sem=x_recv.at[m, e, s],
            device_id={"zero": p}, device_id_type=MESH,
        )

    def arrived(m, e):
        others("zero", me, n, lambda p: swap(m, e, p, p).wait_recv())
        total = parts[0, e, m]
        for s in range(1, n):
            total = total + parts[s, e, m]
        totals[e, m] = total

    def narrow(src, m, e):
        scale = totals[e, m] / d_model
        factor = 1.0 / scale
        scales[...] = scale
        so[m][pl.ds(e, 1), :] = scales[:, pl.ds(pl.multiple_of(me * width, width), width)]

        def body(r, carry):
            at = pl.ds(pl.multiple_of(r * STEP, STEP), STEP)
            for c in range(n):
                lanes = slice(c * width, (c + 1) * width)
                sendbuf[m, e, c, at, :] = (src[at, lanes] * factor[:, lanes]).astype(jnp.bfloat16)
            return carry

        lax.fori_loop(0, rows // STEP, body, 0, unroll=2)

    def place(ref, e, s):
        return ref.at[e, pl.ds(pl.multiple_of(s * rows, rows), rows), :]

    def keep(m, e):
        pltpu.make_async_copy(sendbuf.at[m, e, me], place(o[m], e, me), own_sem.at[m]).start()

    def send(m, e, p):
        pltpu.make_async_remote_copy(
            src_ref=sendbuf.at[m, e, p], dst_ref=place(o[m], e, me),
            send_sem=send_sem.at[m, p], recv_sem=recv_sem.at[m, me],
            device_id={"zero": p}, device_id_type=MESH,
        ).start()

    def send_at(m, e, t):
        @pl.when(me + t < n)
        def _():
            send(m, e, me + t)

        @pl.when(me - t >= 0)
        def _():
            send(m, e, me - t)

    def send_all(m, e):
        for t in range(n - 1, 0, -1):
            send_at(m, e, t)

    depth = rw_ref.shape[1]
    mine = pl.ds(pl.multiple_of(me * depth, depth), depth)
    for copy in small:
        copy.wait()
    rt_ref[bank, :, mine] = (router[...] * gain[...]).astype(jnp.bfloat16)

    def row_copy(s, p):
        at = pl.ds(pl.multiple_of(s * depth, depth), depth)
        return pltpu.make_async_remote_copy(
            src_ref=rt_ref.at[bank, :, at], dst_ref=rt_ref.at[bank, :, at],
            send_sem=rz_send.at[p], recv_sem=rz_recv.at[s],
            device_id={"zero": p}, device_id_type=MESH,
        )

    for i, (m, e) in enumerate(heads):
        head_sizes(m, e)
        if i == 0:
            for later in heads[2:]:
                for c in range(CUTS):
                    head(*later, c).start()
            pl.semaphore_wait(barrier, n - 1 + banks - 1)
        others("zero", me, n, lambda p: swap(m, e, me, p).start())
        if i == 1:
            others("zero", me, n, lambda p: row_copy(me, p).start())

    refill()

    @pl.when(lead)
    def _():
        for k in heads:
            arrived(*k)
            narrow(first.at[k], *k)
            send_all(*k)
            keep(*k)

    def sizes(e, carry):
        slot = lax.rem(e, SLOTS)
        for m in range(2):
            load(m, e, slot).wait()
            acc = sizes_of(stage.at[m, slot], rows, empty)
            sums[e, m] = jnp.sum(acc, axis=0, keepdims=True)

            @pl.when(e + SLOTS < experts)
            def _():
                load(m, e + SLOTS, slot).start()
        return carry

    lax.fori_loop(HEADS, experts, sizes, 0)
    refill()

    span = pl.ds(HEADS, experts - HEADS)
    gates = (n // 2 - 1, n // 2)

    def members(g):
        side = range(n // 2) if g < n // 2 else range(n // 2, n)
        return [(i, p) for i, p in enumerate(p for p in side if p != g)]

    def rise(g, i):
        return pltpu.make_async_remote_copy(
            src_ref=sums.at[span], dst_ref=lower.at[i, span], send_sem=up_send, recv_sem=up_recv.at[i],
            device_id={"zero": g}, device_id_type=MESH,
        )

    def meet(g):
        return pltpu.make_async_remote_copy(
            src_ref=half.at[span], dst_ref=across.at[span], send_sem=mid_send, recv_sem=mid_recv,
            device_id={"zero": n - 1 - g}, device_id_type=MESH,
        )

    def give(i, p):
        return pltpu.make_async_remote_copy(
            src_ref=totals.at[span], dst_ref=totals.at[span], send_sem=down_send.at[i], recv_sem=down_recv,
            device_id={"zero": p}, device_id_type=MESH,
        )

    for g in gates:
        for i, p in members(g):
            @pl.when(me == p)
            def _():
                rise(g, i).start()

    @pl.when(jnp.logical_not(lead))
    def _():
        for k in heads:
            arrived(*k)
            narrow(first.at[k], *k)

    for g in gates:
        @pl.when(me == g)
        def _():
            total = sums[span]
            for i, p in members(g):
                rise(g, i).wait_recv()
                total = total + lower[i, span]
            half[span] = total
            meet(g).start()
            meet(g).wait_recv()
            totals[span] = half[span] + across[span]
            for i, p in members(g):
                give(i, p).start()

        for i, p in members(g):
            @pl.when(me == p)
            def _():
                give(i, p).wait_recv()

    def put(m, d):
        return pltpu.make_async_copy(
            sendbuf.at[m, pl.ds(main, TAIL), lax.rem(me + d, n)], tails[d].at[m], tail_sem.at[d, m]
        )

    def narrowed(e, carry):
        slot = lax.rem(e, SLOTS)
        for m in range(2):
            load(m, e, slot).wait()
            narrow(stage.at[m, slot], m, e)

            @pl.when(e + SLOTS < experts)
            def _():
                load(m, e + SLOTS, slot).start()

            @pl.when(e < main)
            def _():
                keep(m, e)

                @pl.when(lead)
                def _():
                    send_at(m, e, 1)
        return carry

    lax.fori_loop(HEADS, experts, narrowed, 0)
    for m in range(2):
        for d in range(n):
            put(m, d).start()

    @pl.when(jnp.logical_not(lead))
    def _():
        for k in heads:
            send_all(*k)
            keep(*k)

        def near(e, carry):
            for m in range(2):
                send_at(m, e, 1)
            return carry

        lax.fori_loop(HEADS, main, near, 0)

    def far(e, carry):
        for m in range(2):
            for t in range(2, n):
                send_at(m, e, t)
        return carry

    lax.fori_loop(HEADS, main, far, 0)
    for m in range(2):
        for d in range(n):
            put(m, d).wait()

    others("zero", me, n, lambda p: row_copy(p, p).wait_recv())

    def column_copy(s, p):
        return pltpu.make_async_remote_copy(
            src_ref=rt_ref.at[s], dst_ref=rt_ref.at[s],
            send_sem=rb_send.at[p], recv_sem=rb_recv.at[s],
            device_id={"bank": p}, device_id_type=MESH,
        )

    others("bank", bank, banks, lambda p: column_copy(bank, p).start())
    others("bank", bank, banks, lambda p: column_copy(p, p).wait_recv())
    others("bank", bank, banks, lambda p: column_copy(bank, p).wait_send())
    others("zero", me, n, lambda p: row_copy(me, p).wait_send())
    for m, e in heads:
        others("zero", me, n, lambda p: swap(m, e, me, p).wait_send())
    for g in gates:
        @pl.when(me == g)
        def _():
            meet(g).wait_send()
            for i, p in members(g):
                give(i, p).wait_send()

        for i, p in members(g):
            @pl.when(me == p)
            def _():
                rise(g, i).wait_send()

    for m in range(2):
        def whole(s, p):
            return pltpu.make_async_remote_copy(
                src_ref=sendbuf.at[m, pl.ds(0, main), p],
                dst_ref=o[m].at[:, pl.ds(pl.multiple_of(s * rows, rows), rows), :],
                send_sem=send_sem.at[m, p], recv_sem=recv_sem.at[m, s],
                device_id={"zero": p}, device_id_type=MESH,
            )

        pltpu.make_async_copy(
            sendbuf.at[m, pl.ds(0, main), me], o[m].at[:, pl.ds(pl.multiple_of(me * rows, rows), rows), :], own_sem.at[m]
        ).wait()
        others("zero", me, n, lambda p: whole(me, p).wait_send())
        others("zero", me, n, lambda p: whole(p, p).wait_recv())


def copy_kernel(n, a_ref, b_ref, own_ref, sa_ref, sb_ref, rt_ref, *outs):
    c_ref, d_ref = outs[:2]
    e = pl.program_id(0)
    tail, rows = own_ref.shape[1:3]
    main = pl.num_programs(0) - tail

    @pl.when(e < main)
    def _():
        c_ref[...] = a_ref[...]
        d_ref[...] = b_ref[...]

    @pl.when(e == 0)
    def _():
        for src, dst in zip((sa_ref, sb_ref, rt_ref), outs[2:]):
            dst[...] = src[...]

    @pl.when(e >= main)
    def _():
        at = pl.ds(pl.multiple_of(lax.axis_index("zero") * rows, rows), rows)
        c_ref[0, at, :] = own_ref[0, e - main]
        d_ref[0, at, :] = own_ref[1, e - main]


def spread(n, og, ou, own, *small):
    main, height, width = og.shape
    block = pl.BlockSpec((1, height, width), lambda e: (e, 0, 0))
    front = pl.BlockSpec((1, height, width), lambda e: (jnp.minimum(e, main - 1), 0, 0))
    experts = main + own.shape[1]
    out = jax.ShapeDtypeStruct((experts, height, width), og.dtype)

    def all_of(a):
        return pl.BlockSpec(a.shape, lambda e: (0,) * a.ndim)

    return pl.pallas_call(
        functools.partial(copy_kernel, n),
        grid=(experts,),
        in_specs=[front, front] + [all_of(a) for a in (own, *small)],
        out_specs=(block, block, *[all_of(a) for a in small]),
        out_shape=(out, out, *[jax.ShapeDtypeStruct(a.shape, a.dtype) for a in small]),
        cost_estimate=pl.CostEstimate(flops=0, bytes_accessed=8 * og.size, transcendentals=0),
        name="spread",
    )(og, ou, own, *small)


def join_kernel(n, shifts, *refs):
    count = len(shifts)
    blocks, outs, sem = refs[2 : 2 + count], refs[2 + count : 4 + count], refs[4 + count]
    me = lax.axis_index("zero")
    tail, rows = blocks[0].shape[1:3]
    ends = pl.ds(outs[0].shape[0] - tail, tail)
    copies = []
    for i, d in enumerate(shifts):
        at = pl.ds(pl.multiple_of(lax.rem(me - d + n, n) * rows, rows), rows)
        for m in range(2):
            copies.append(pltpu.make_async_copy(blocks[i].at[m], outs[m].at[ends, at, :], sem.at[i, m]))
    for copy in copies:
        copy.start()
    for copy in copies:
        copy.wait()


def join(n, shifts, og, ou, blocks):
    anywhere = pl.BlockSpec(memory_space=pl.ANY)
    vmem = pl.BlockSpec(memory_space=pltpu.VMEM)
    return pl.pallas_call(
        functools.partial(join_kernel, n, shifts),
        out_shape=(jax.ShapeDtypeStruct(og.shape, og.dtype), jax.ShapeDtypeStruct(ou.shape, ou.dtype)),
        in_specs=[anywhere, anywhere] + [vmem] * len(blocks),
        out_specs=(anywhere, anywhere),
        scratch_shapes=[pltpu.SemaphoreType.DMA((len(blocks), 2))],
        input_output_aliases={0: 0, 1: 1},
        compiler_params=pltpu.CompilerParams(vmem_limit_bytes=8 * 1024 * 1024),
        name="join",
    )(og, ou, *blocks)


def local(n, banks, w_gate, w_up, router_weight, router_gain):
    experts, rows, cols = w_gate.shape
    width = cols // n
    depth, heads = router_weight.shape
    fits = width % 128 == 0 and rows % (8 * CUTS) == 0 and depth % 128 == 0 and heads % 16 == 0
    fits = fits and experts > HEADS + TAIL and n % 2 == 0
    if not fits:
        return plain(n, w_gate, w_up, router_weight, router_gain)
    anywhere = pl.BlockSpec(memory_space=pl.ANY)
    vmem = pl.BlockSpec(memory_space=pltpu.VMEM)
    dma = pltpu.SemaphoreType.DMA
    serve = jax.ShapeDtypeStruct((experts - TAIL, rows * n, width), jnp.bfloat16)
    tail = jax.ShapeDtypeStruct((2, TAIL, rows, width), jnp.bfloat16)
    scale = jax.ShapeDtypeStruct((experts, width), jnp.float32)
    sizes = pltpu.VMEM((experts, 2, 1, cols), jnp.float32)
    og, ou, sg, su, rt, *tails = pl.pallas_call(
        functools.partial(kernel, n, banks),
        out_shape=(serve, serve, scale, scale, jax.ShapeDtypeStruct((banks, heads, depth * n), jnp.bfloat16), *[tail] * n),
        in_specs=[anywhere] * 4,
        out_specs=(anywhere, anywhere, vmem, vmem, vmem, *[anywhere] * n),
        scratch_shapes=[
            pltpu.VMEM((2, SLOTS, rows, cols), jnp.float32),
            pltpu.VMEM((2, HEADS, rows, cols), jnp.float32),
            pltpu.VMEM((2, experts, n, rows, width), jnp.bfloat16),
            pltpu.VMEM((n, HEADS, 2, 1, cols), jnp.float32),
            sizes,
            pltpu.VMEM((max(n // 2 - 1, 1), experts, 2, 1, cols), jnp.float32),
            sizes, sizes, sizes,
            pltpu.VMEM((1, cols), jnp.float32),
            pltpu.VMEM((heads, depth), jnp.float32),
            pltpu.VMEM((1, depth), jnp.float32),
            dma((n, 2)), dma((2, SLOTS)), dma((2, HEADS, CUTS)), dma((2,)), dma((2, n)), dma((2, n)),
            dma((2, HEADS, n)), dma((2, HEADS, n)), dma, dma((n,)), dma, dma, dma((n,)), dma,
            dma((n,)), dma((n,)), dma((banks,)), dma((banks,)), dma((2,)),
        ],
        compiler_params=pltpu.CompilerParams(
            collective_id=0, has_side_effects=True, vmem_limit_bytes=58 * 1024 * 1024
        ),
    )(w_gate, w_up, router_weight.T, router_gain[None, :])
    arrived = [
        lax.ppermute(tails[d], "zero", [(i, (i + d) % n) for i in range(n)]) for d in range(1, n)
    ]
    og, ou, sg, su, rt = spread(n, og, ou, tails[0], sg, su, rt)
    if n > 2:
        og, ou = join(n, (1,), og, ou, arrived[:1])
    og, ou = join(n, tuple(range(2, n)) or (1,), og, ou, arrived[1:] or arrived)
    return og, ou, sg, su, rt.reshape(banks * heads, depth * n).T


def solution(mesh):
    n, banks = mesh.shape["zero"], mesh.shape["bank"]
    return jax.shard_map(
        functools.partial(local, n, banks),
        mesh=mesh,
        in_specs=(
            P(("trial", "bank"), "zero", None),
            P(("trial", "bank"), "zero", None),
            P(("trial", "zero"), "bank"),
            P(("trial", "zero")),
        ),
        out_specs=(
            P(("trial", "bank"), None, "zero"),
            P(("trial", "bank"), None, "zero"),
            P(("trial", "bank"), "zero"),
            P(("trial", "bank"), "zero"),
            P("trial", None),
        ),
        check_vma=False,
    )
```

```python
import functools

import jax
import jax.numpy as jnp
from jax import lax
from jax.experimental import pallas as pl
from jax.experimental.pallas import tpu as pltpu
from jax.sharding import PartitionSpec as P

MESH = pl.DeviceIdType.MESH
SLOTS = 3
STEP = 16
CUTS = 4
HEADS = 2
TAIL = 2


def plain(n, w_gate, w_up, router_weight, router_gain):
    d_model = w_gate.shape[1] * n

    def rescaled(w):
        scale = lax.psum(jnp.sum(jnp.abs(w), axis=1), "zero") / d_model
        narrow = (w / jnp.expand_dims(scale, 1)).astype(jnp.bfloat16)
        serve = lax.all_to_all(narrow, "zero", split_axis=2, concat_axis=1, tiled=True)
        width = serve.shape[2]
        return serve, lax.dynamic_slice_in_dim(scale, lax.axis_index("zero") * width, width, axis=1)

    serve_gate, scale_gate = rescaled(w_gate)
    serve_up, scale_up = rescaled(w_up)
    part = (router_weight * router_gain[:, None]).astype(jnp.bfloat16)
    row = lax.all_gather(part, "zero", axis=0, tiled=True)
    router = lax.all_gather(row, "bank", axis=1, tiled=True)
    return serve_gate, serve_up, scale_gate, scale_up, router


def kernel(
    n, banks, wg_ref, wu_ref, rw_ref, rg_ref, *refs
):
    og_ref, ou_ref, sg_ref, su_ref, rt_ref = refs[:5]
    tails = refs[5 : 5 + n]
    stage, first, sendbuf, parts, sums, lower, half, across, totals, scales, router, gain = refs[5 + n : 17 + n]
    (
    tail_sem, in_sem, first_sem, own_sem, send_sem, recv_sem, x_send, x_recv, up_send, up_recv, mid_send, mid_recv,
    down_send, down_recv, rz_send, rz_recv, rb_send, rb_recv, r_sem,
    ) = refs[17 + n :]
    me = lax.axis_index("zero")
    bank = lax.axis_index("bank")
    lead = lax.rem(lax.axis_index("trial"), 2) == 1
    w, o, so = (wg_ref, wu_ref), (og_ref, ou_ref), (sg_ref, su_ref)
    experts, rows, cols = wg_ref.shape
    width = cols // n
    d_model = rows * n
    main = experts - TAIL
    piece = rows // CUTS
    heads = [(m, e) for e in range(HEADS) for m in range(2)]

    def head(m, e, c):
        at = pl.ds(c * piece, piece)
        return pltpu.make_async_copy(w[m].at[e, at], first.at[m, e, at], first_sem.at[m, e, c])

    def load(m, e, slot):
        return pltpu.make_async_copy(w[m].at[e], stage.at[m, slot], in_sem.at[m, slot])

    def refill():
        for e in range(HEADS, min(HEADS + SLOTS, experts)):
            for m in range(2):
                load(m, e, e % SLOTS).start()

    for m, e in heads[:2]:
        for c in range(CUTS):
            head(m, e, c).start()
    small = [pltpu.make_async_copy(src, dst, r_sem.at[i]) for i, (src, dst) in enumerate(((rw_ref, router), (rg_ref, gain)))]
    for copy in small:
        copy.start()

    def others(axis, here, count, act):
        for p in range(count):
            @pl.when(here != p)
            def _():
                act(p)

    barrier = pltpu.get_barrier_semaphore()

    def greet(axis):
        return lambda p: pl.semaphore_signal(barrier, inc=1, device_id={axis: p}, device_id_type=MESH)

    others("zero", me, n, greet("zero"))
    others("bank", bank, banks, greet("bank"))

    def sizes_of(src, count, acc):
        def body(r, acc):
            return acc + jnp.abs(src[pl.ds(pl.multiple_of(r * 8, 8), 8), :])

        return lax.fori_loop(0, count // 8, body, acc, unroll=8)

    empty = jnp.zeros((8, cols), jnp.float32)

    def head_sizes(m, e):
        acc = empty
        for c in range(CUTS):
            head(m, e, c).wait()
            acc = sizes_of(first.at[m, e, pl.ds(c * piece, piece)], piece, acc)
        parts[me, e, m] = jnp.sum(acc, axis=0, keepdims=True)

    def swap(m, e, s, p):
        return pltpu.make_async_remote_copy(
            src_ref=parts.at[s, e, m], dst_ref=parts.at[s, e, m],
            send_sem=x_send.at[m, e, p], recv_sem=x_recv.at[m, e, s],
            device_id={"zero": p}, device_id_type=MESH,
        )

    def arrived(m, e):
        others("zero", me, n, lambda p: swap(m, e, p, p).wait_recv())
        total = parts[0, e, m]
        for s in range(1, n):
            total = total + parts[s, e, m]
        totals[e, m] = total

    def narrow(src, m, e):
        scale = totals[e, m] / d_model
        factor = 1.0 / scale
        scales[...] = scale
        so[m][pl.ds(e, 1), :] = scales[:, pl.ds(pl.multiple_of(me * width, width), width)]

        def body(r, carry):
            at = pl.ds(pl.multiple_of(r * STEP, STEP), STEP)
            for c in range(n):
                lanes = slice(c * width, (c + 1) * width)
                sendbuf[m, e, c, at, :] = (src[at, lanes] * factor[:, lanes]).astype(jnp.bfloat16)
            return carry

        lax.fori_loop(0, rows // STEP, body, 0, unroll=2)

    def place(ref, e, s):
        return ref.at[e, pl.ds(pl.multiple_of(s * rows, rows), rows), :]

    def keep(m, e):
        pltpu.make_async_copy(sendbuf.at[m, e, me], place(o[m], e, me), own_sem.at[m]).start()

    def send(m, e, p):
        pltpu.make_async_remote_copy(
            src_ref=sendbuf.at[m, e, p], dst_ref=place(o[m], e, me),
            send_sem=send_sem.at[m, p], recv_sem=recv_sem.at[m, me],
            device_id={"zero": p}, device_id_type=MESH,
        ).start()

    def send_at(m, e, t):
        @pl.when(me + t < n)
        def _():
            send(m, e, me + t)

        @pl.when(me - t >= 0)
        def _():
            send(m, e, me - t)

    def send_all(m, e):
        for t in range(n - 1, 0, -1):
            send_at(m, e, t)

    depth = rw_ref.shape[1]
    mine = pl.ds(pl.multiple_of(me * depth, depth), depth)
    for copy in small:
        copy.wait()
    rt_ref[bank, :, mine] = (router[...] * gain[...]).astype(jnp.bfloat16)

    def row_copy(s, p):
        at = pl.ds(pl.multiple_of(s * depth, depth), depth)
        return pltpu.make_async_remote_copy(
            src_ref=rt_ref.at[bank, :, at], dst_ref=rt_ref.at[bank, :, at],
            send_sem=rz_send.at[p], recv_sem=rz_recv.at[s],
            device_id={"zero": p}, device_id_type=MESH,
        )

    for i, (m, e) in enumerate(heads):
        head_sizes(m, e)
        if i == 0:
            for later in heads[2:]:
                for c in range(CUTS):
                    head(*later, c).start()
            pl.semaphore_wait(barrier, n - 1 + banks - 1)
        others("zero", me, n, lambda p: swap(m, e, me, p).start())
        if i == 1:
            others("zero", me, n, lambda p: row_copy(me, p).start())

    refill()

    @pl.when(lead)
    def _():
        for k in heads:
            arrived(*k)
            narrow(first.at[k], *k)
            send_all(*k)
            keep(*k)

    def sizes(e, carry):
        slot = lax.rem(e, SLOTS)
        for m in range(2):
            load(m, e, slot).wait()
            acc = sizes_of(stage.at[m, slot], rows, empty)
            sums[e, m] = jnp.sum(acc, axis=0, keepdims=True)

            @pl.when(e + SLOTS < experts)
            def _():
                load(m, e + SLOTS, slot).start()
        return carry

    lax.fori_loop(HEADS, experts, sizes, 0)
    refill()

    span = pl.ds(HEADS, experts - HEADS)
    gates = (n // 2 - 1, n // 2)

    def members(g):
        side = range(n // 2) if g < n // 2 else range(n // 2, n)
        return [(i, p) for i, p in enumerate(p for p in side if p != g)]

    def rise(g, i):
        return pltpu.make_async_remote_copy(
            src_ref=sums.at[span], dst_ref=lower.at[i, span], send_sem=up_send, recv_sem=up_recv.at[i],
            device_id={"zero": g}, device_id_type=MESH,
        )

    def meet(g):
        return pltpu.make_async_remote_copy(
            src_ref=half.at[span], dst_ref=across.at[span], send_sem=mid_send, recv_sem=mid_recv,
            device_id={"zero": n - 1 - g}, device_id_type=MESH,
        )

    def give(i, p):
        return pltpu.make_async_remote_copy(
            src_ref=totals.at[span], dst_ref=totals.at[span], send_sem=down_send.at[i], recv_sem=down_recv,
            device_id={"zero": p}, device_id_type=MESH,
        )

    for g in gates:
        for i, p in members(g):
            @pl.when(me == p)
            def _():
                rise(g, i).start()

    @pl.when(jnp.logical_not(lead))
    def _():
        for k in heads:
            arrived(*k)
            narrow(first.at[k], *k)

    for g in gates:
        @pl.when(me == g)
        def _():
            total = sums[span]
            for i, p in members(g):
                rise(g, i).wait_recv()
                total = total + lower[i, span]
            half[span] = total
            meet(g).start()
            meet(g).wait_recv()
            totals[span] = half[span] + across[span]
            for i, p in members(g):
                give(i, p).start()

        for i, p in members(g):
            @pl.when(me == p)
            def _():
                give(i, p).wait_recv()

    @pl.when(jnp.logical_not(lead))
    def _():
        for k in heads:
            send_all(*k)
            keep(*k)

    def put(m, d):
        return pltpu.make_async_copy(
            sendbuf.at[m, pl.ds(main, TAIL), lax.rem(me + d, n)], tails[d].at[m], tail_sem.at[d, m]
        )

    def narrowed(e, carry):
        slot = lax.rem(e, SLOTS)
        for m in range(2):
            load(m, e, slot).wait()
            narrow(stage.at[m, slot], m, e)

            @pl.when(e + SLOTS < experts)
            def _():
                load(m, e + SLOTS, slot).start()

            @pl.when(e < main)
            def _():
                keep(m, e)

                @pl.when(lead)
                def _():
                    send_at(m, e, 1)
        return carry

    lax.fori_loop(HEADS, experts, narrowed, 0)
    for m in range(2):
        for d in range(n):
            put(m, d).start()

    @pl.when(jnp.logical_not(lead))
    def _():
        def near(e, carry):
            for m in range(2):
                send_at(m, e, 1)
            return carry

        lax.fori_loop(HEADS, main, near, 0)

    def far(e, carry):
        for m in range(2):
            for t in range(2, n):
                send_at(m, e, t)
        return carry

    lax.fori_loop(HEADS, main, far, 0)
    for m in range(2):
        for d in range(n):
            put(m, d).wait()

    others("zero", me, n, lambda p: row_copy(p, p).wait_recv())

    def column_copy(s, p):
        return pltpu.make_async_remote_copy(
            src_ref=rt_ref.at[s], dst_ref=rt_ref.at[s],
            send_sem=rb_send.at[p], recv_sem=rb_recv.at[s],
            device_id={"bank": p}, device_id_type=MESH,
        )

    others("bank", bank, banks, lambda p: column_copy(bank, p).start())
    others("bank", bank, banks, lambda p: column_copy(p, p).wait_recv())
    others("bank", bank, banks, lambda p: column_copy(bank, p).wait_send())
    others("zero", me, n, lambda p: row_copy(me, p).wait_send())
    for m, e in heads:
        others("zero", me, n, lambda p: swap(m, e, me, p).wait_send())
    for g in gates:
        @pl.when(me == g)
        def _():
            meet(g).wait_send()
            for i, p in members(g):
                give(i, p).wait_send()

        for i, p in members(g):
            @pl.when(me == p)
            def _():
                rise(g, i).wait_send()

    for m in range(2):
        def whole(s, p):
            return pltpu.make_async_remote_copy(
                src_ref=sendbuf.at[m, pl.ds(0, main), p],
                dst_ref=o[m].at[:, pl.ds(pl.multiple_of(s * rows, rows), rows), :],
                send_sem=send_sem.at[m, p], recv_sem=recv_sem.at[m, s],
                device_id={"zero": p}, device_id_type=MESH,
            )

        pltpu.make_async_copy(
            sendbuf.at[m, pl.ds(0, main), me], o[m].at[:, pl.ds(pl.multiple_of(me * rows, rows), rows), :], own_sem.at[m]
        ).wait()
        others("zero", me, n, lambda p: whole(me, p).wait_send())
        others("zero", me, n, lambda p: whole(p, p).wait_recv())


def copy_kernel(n, a_ref, b_ref, own_ref, sa_ref, sb_ref, rt_ref, *outs):
    c_ref, d_ref = outs[:2]
    e = pl.program_id(0)
    tail, rows = own_ref.shape[1:3]
    main = pl.num_programs(0) - tail

    @pl.when(e < main)
    def _():
        c_ref[...] = a_ref[...]
        d_ref[...] = b_ref[...]

    @pl.when(e == 0)
    def _():
        for src, dst in zip((sa_ref, sb_ref, rt_ref), outs[2:]):
            dst[...] = src[...]

    @pl.when(e >= main)
    def _():
        at = pl.ds(pl.multiple_of(lax.axis_index("zero") * rows, rows), rows)
        c_ref[0, at, :] = own_ref[0, e - main]
        d_ref[0, at, :] = own_ref[1, e - main]


def spread(n, og, ou, own, *small):
    main, height, width = og.shape
    block = pl.BlockSpec((1, height, width), lambda e: (e, 0, 0))
    front = pl.BlockSpec((1, height, width), lambda e: (jnp.minimum(e, main - 1), 0, 0))
    experts = main + own.shape[1]
    out = jax.ShapeDtypeStruct((experts, height, width), og.dtype)

    def all_of(a):
        return pl.BlockSpec(a.shape, lambda e: (0,) * a.ndim)

    return pl.pallas_call(
        functools.partial(copy_kernel, n),
        grid=(experts,),
        in_specs=[front, front] + [all_of(a) for a in (own, *small)],
        out_specs=(block, block, *[all_of(a) for a in small]),
        out_shape=(out, out, *[jax.ShapeDtypeStruct(a.shape, a.dtype) for a in small]),
        cost_estimate=pl.CostEstimate(flops=0, bytes_accessed=8 * og.size, transcendentals=0),
        name="spread",
    )(og, ou, own, *small)


def join_kernel(n, shifts, *refs):
    count = len(shifts)
    blocks, outs, sem = refs[2 : 2 + count], refs[2 + count : 4 + count], refs[4 + count]
    me = lax.axis_index("zero")
    tail, rows = blocks[0].shape[1:3]
    ends = pl.ds(outs[0].shape[0] - tail, tail)
    copies = []
    for i, d in enumerate(shifts):
        at = pl.ds(pl.multiple_of(lax.rem(me - d + n, n) * rows, rows), rows)
        for m in range(2):
            copies.append(pltpu.make_async_copy(blocks[i].at[m], outs[m].at[ends, at, :], sem.at[i, m]))
    for copy in copies:
        copy.start()
    for copy in copies:
        copy.wait()


def join(n, shifts, og, ou, blocks):
    anywhere = pl.BlockSpec(memory_space=pl.ANY)
    vmem = pl.BlockSpec(memory_space=pltpu.VMEM)
    return pl.pallas_call(
        functools.partial(join_kernel, n, shifts),
        out_shape=(jax.ShapeDtypeStruct(og.shape, og.dtype), jax.ShapeDtypeStruct(ou.shape, ou.dtype)),
        in_specs=[anywhere, anywhere] + [vmem] * len(blocks),
        out_specs=(anywhere, anywhere),
        scratch_shapes=[pltpu.SemaphoreType.DMA((len(blocks), 2))],
        input_output_aliases={0: 0, 1: 1},
        compiler_params=pltpu.CompilerParams(vmem_limit_bytes=8 * 1024 * 1024),
        name="join",
    )(og, ou, *blocks)


def local(n, banks, w_gate, w_up, router_weight, router_gain):
    experts, rows, cols = w_gate.shape
    width = cols // n
    depth, heads = router_weight.shape
    fits = width % 128 == 0 and rows % (8 * CUTS) == 0 and depth % 128 == 0 and heads % 16 == 0
    fits = fits and experts > HEADS + TAIL and n % 2 == 0
    if not fits:
        return plain(n, w_gate, w_up, router_weight, router_gain)
    anywhere = pl.BlockSpec(memory_space=pl.ANY)
    vmem = pl.BlockSpec(memory_space=pltpu.VMEM)
    dma = pltpu.SemaphoreType.DMA
    serve = jax.ShapeDtypeStruct((experts - TAIL, rows * n, width), jnp.bfloat16)
    tail = jax.ShapeDtypeStruct((2, TAIL, rows, width), jnp.bfloat16)
    scale = jax.ShapeDtypeStruct((experts, width), jnp.float32)
    sizes = pltpu.VMEM((experts, 2, 1, cols), jnp.float32)
    og, ou, sg, su, rt, *tails = pl.pallas_call(
        functools.partial(kernel, n, banks),
        out_shape=(serve, serve, scale, scale, jax.ShapeDtypeStruct((banks, heads, depth * n), jnp.bfloat16), *[tail] * n),
        in_specs=[anywhere] * 4,
        out_specs=(anywhere, anywhere, vmem, vmem, vmem, *[anywhere] * n),
        scratch_shapes=[
            pltpu.VMEM((2, SLOTS, rows, cols), jnp.float32),
            pltpu.VMEM((2, HEADS, rows, cols), jnp.float32),
            pltpu.VMEM((2, experts, n, rows, width), jnp.bfloat16),
            pltpu.VMEM((n, HEADS, 2, 1, cols), jnp.float32),
            sizes,
            pltpu.VMEM((max(n // 2 - 1, 1), experts, 2, 1, cols), jnp.float32),
            sizes, sizes, sizes,
            pltpu.VMEM((1, cols), jnp.float32),
            pltpu.VMEM((heads, depth), jnp.float32),
            pltpu.VMEM((1, depth), jnp.float32),
            dma((n, 2)), dma((2, SLOTS)), dma((2, HEADS, CUTS)), dma((2,)), dma((2, n)), dma((2, n)),
            dma((2, HEADS, n)), dma((2, HEADS, n)), dma, dma((n,)), dma, dma, dma((n,)), dma,
            dma((n,)), dma((n,)), dma((banks,)), dma((banks,)), dma((2,)),
        ],
        compiler_params=pltpu.CompilerParams(
            collective_id=0, has_side_effects=True, vmem_limit_bytes=58 * 1024 * 1024
        ),
    )(w_gate, w_up, router_weight.T, router_gain[None, :])
    arrived = [
        lax.ppermute(tails[d], "zero", [(i, (i + d) % n) for i in range(n)]) for d in range(1, n)
    ]
    og, ou, sg, su, rt = spread(n, og, ou, tails[0], sg, su, rt)
    if n > 2:
        og, ou = join(n, (1,), og, ou, arrived[:1])
    og, ou = join(n, tuple(range(2, n)) or (1,), og, ou, arrived[1:] or arrived)
    return og, ou, sg, su, rt.reshape(banks * heads, depth * n).T


def solution(mesh):
    n, banks = mesh.shape["zero"], mesh.shape["bank"]
    return jax.shard_map(
        functools.partial(local, n, banks),
        mesh=mesh,
        in_specs=(
            P(("trial", "bank"), "zero", None),
            P(("trial", "bank"), "zero", None),
            P(("trial", "zero"), "bank"),
            P(("trial", "zero")),
        ),
        out_specs=(
            P(("trial", "bank"), None, "zero"),
            P(("trial", "bank"), None, "zero"),
            P(("trial", "bank"), "zero"),
            P(("trial", "bank"), "zero"),
            P("trial", None),
        ),
        check_vma=False,
    )
```
